32 devices in a mesh: dp: 8 (over z, x), mp: 4 (over y, core).
Axes of the slice: x: 2, y: 2, z: 4, core: 2. Of those that a mesh axis runs over, the one named last changes fastest.
Arguments:
- acts: bfloat16 [2048, 4096], P('dp'), may hold values from -6 to 6
- cotangent: bfloat16 [2048, 2048], P('dp', 'mp'), may hold values from -0.13183594 to 0.13183594
- stats: float32 [4, 8, 2, 512, 512], P('mp', 'dp'), as said below
- owner_slot: int32 [8], replicated, may hold values from 0 to 7, as said below
Outputs:
- update: bfloat16 [8, 512, 2048], P(None, 'dp', 'mp')
- new_stats: float32 [4, 8, 2, 512, 512], P('mp', 'dp')
The draws below stay inside these ranges and needn't reach their ends.
Inputs may be any that keep to these rules, and one draw needn't show every extreme that they name: Distinct slot numbers; row block w is held by device owner_slot[w] // 1 of dp at its position owner_slot[w] % 1; some device holds 1 block. Every stats[j, s, f] is a symmetric positive definite matrix.
All inputs are finite; a program needn't handle non-finite values.
Results may differ from the reference program's by a relative error of at most 0.012.
The reference program's roundings to bfloat16 on the way (of `gradient`) count: a program that leaves them out, or rounds other values in their place, can miss the bound.
Values may be sent and summed in bfloat16 or wider, within the bound.
A program may use at most 192 MiB of HBM per device.

```python
import jax
import jax.numpy as jnp
from jax import lax

BLK = 512
SLOTS = 1
ITERS = 5
RB = 8
HID = 4096
COLS = 2048
TOKENS = 2048
N_DP = 8
N_MP = 4


def draw_stats(key, part):
    full_shape = (N_MP, N_DP * SLOTS, 2, BLK, BLK)
    key_off, key_diag = jax.random.split(jax.random.fold_in(key, 11), 2)
    off_noise = 0.1 * jax.random.normal(key_off, full_shape, jnp.float32)
    symmetric = 0.5 * (off_noise + jnp.swapaxes(off_noise, -1, -2))
    identity = jnp.eye(BLK, dtype=jnp.float32)
    off_part = symmetric * (1.0 - identity)
    row_weight = jnp.sum(jnp.abs(off_part), axis=-1)
    dominance = jax.random.uniform(key_diag, full_shape[:-1], jnp.float32, 1.05, 2.0)
    matrix = off_part + identity * (row_weight * dominance)[..., None]
    return matrix


def draw_owner_slot(key, part):
    key_devices, key_places, key_order = jax.random.split(jax.random.fold_in(key, 23), 3)
    holders = RB - SLOTS + 1
    devices = jax.random.permutation(key_devices, N_DP)[:holders].astype(jnp.int32)
    places = jax.random.randint(key_places, (holders,), 0, SLOTS).astype(jnp.int32)
    first_owner = devices[0] * SLOTS + jnp.arange(SLOTS, dtype=jnp.int32)
    other_owners = devices[1:] * SLOTS + places[1:]
    slot_list = jnp.concatenate([first_owner, other_owners])
    shuffle = jax.random.permutation(key_order, RB)
    return slot_list[shuffle].astype(jnp.int32)


def block_scale(rng, shape, shards, smallest, largest):
    loudness = 1.0
    for dim, parts in shards:
        draws = jax.random.uniform(jax.random.fold_in(jax.random.fold_in(rng, 6), dim), (parts,), jnp.float32, smallest / len(shards), largest / len(shards))
        loudness = loudness * jnp.repeat(jnp.exp(draws), shape[dim] // parts).reshape((-1,) + (1,) * (len(shape) - 1 - dim))
    return loudness


def centred(own_key, extent, width, bound, cuts=(), kind=jnp.bfloat16):
    level = block_scale(own_key, extent, cuts, -0.22, 0.18) if cuts else 1.0
    values = jax.random.normal(own_key, extent, jnp.float32) * width * level
    return jnp.minimum(jnp.maximum(values, -bound), bound).astype(kind)


def setup_inputs(seed: int = 0) -> dict:
    streams_of = jax.random.split(jax.random.key(seed), 5)
    return {
        "acts": centred(streams_of[0], (TOKENS, HID), 1.0, 6.0, ((0, 8),)),
        "cotangent": centred(streams_of[1], (TOKENS, COLS), (1.0 / TOKENS ** 0.5), 0.13183594, ((0, 8), (1, 4))),
        "stats": draw_stats(jax.random.fold_in(streams_of[4], 71), 0),
        "owner_slot": draw_owner_slot(jax.random.fold_in(streams_of[4], 71), 0),
    }


BETA = 0.9
DAMPING = 0.001
EPSILON = 1e-06

def matmul(former, latter):
    return jnp.dot(former.astype(jnp.bfloat16), latter.astype(jnp.bfloat16), preferred_element_type=jnp.float32)

def inverse_root(statistic):
    identity = jnp.eye(statistic.shape[0], dtype=jnp.float32)
    damped = statistic + DAMPING * identity
    frob_norm = jnp.sqrt(jnp.sum(damped * damped) + EPSILON)
    moment = damped / frob_norm
    result = identity
    for iteration in range(ITERS):
        factor = (5.0 * identity - moment) * 0.25
        if iteration == 0:
            result = factor
        else:
            result = matmul(result, factor)
        if iteration + 1 < ITERS:
            square = matmul(factor, factor)
            moment = matmul(square, matmul(square, moment))
    return result * frob_norm ** (-0.25)

def precondition(grad_block, stat_pair):
    gram_left = jnp.dot(grad_block, grad_block.T, preferred_element_type=jnp.float32)
    gram_right = jnp.dot(grad_block.T, grad_block, preferred_element_type=jnp.float32)
    fresh_left = BETA * stat_pair[0] + (1.0 - BETA) * gram_left
    fresh_right = BETA * stat_pair[1] + (1.0 - BETA) * gram_right
    root_left = inverse_root(fresh_left)
    root_right = inverse_root(fresh_right)
    direction = matmul(matmul(root_left, grad_block), root_right)
    grad_wide = grad_block.astype(jnp.float32)
    graft_ratio = jnp.sqrt((jnp.mean(grad_wide * grad_wide) + EPSILON) / (jnp.mean(direction * direction) + EPSILON))
    return ((direction * graft_ratio).astype(jnp.bfloat16), jnp.stack([fresh_left, fresh_right]))

def reference(acts, cotangent, stats, owner_slot):
    gradient = jnp.dot(acts.T, cotangent, preferred_element_type=jnp.float32).astype(jnp.bfloat16)
    update = jnp.zeros((HID, COLS), jnp.bfloat16)
    zero_index = jnp.zeros((), jnp.int32)

    def one_block(counter, carry):
        stat_store, update_store = carry
        shard = (counter // RB).astype(jnp.int32)
        block_id = (counter % RB).astype(jnp.int32)
        row_start = (block_id * BLK).astype(jnp.int32)
        col_start = (shard * BLK).astype(jnp.int32)
        grad_block = lax.dynamic_slice(gradient, (row_start, col_start), (BLK, BLK))
        slot_id = owner_slot[block_id].astype(jnp.int32)
        stat_pair = lax.dynamic_slice(stat_store, (shard, slot_id, zero_index, zero_index, zero_index), (1, 1, 2, BLK, BLK))[0, 0]
        direction, fresh = precondition(grad_block, stat_pair)
        stat_store = lax.dynamic_update_slice(stat_store, fresh[None, None], (shard, slot_id, zero_index, zero_index, zero_index))
        update_store = lax.dynamic_update_slice(update_store, direction, (row_start, col_start))
        return (stat_store, update_store)
    new_stats, update = lax.fori_loop(0, N_MP * RB, one_block, (stats, update))
    return (update.reshape(RB, BLK, COLS), new_stats)
```

```python
import jax
import jax.numpy as jnp
from jax import lax
from jax.experimental import pallas as pl
from jax.experimental.pallas import tpu as pltpu
from jax.sharding import PartitionSpec as P

ITERS = 5


BETA = 0.9
DAMPING = 0.001
EPSILON = 1e-06


def batched(former, latter):
    return jnp.einsum(
        "kij,kjl->kil",
        former.astype(jnp.bfloat16),
        latter.astype(jnp.bfloat16),
        preferred_element_type=jnp.float32,
    )


def inverse_roots(stat_pair):
    identity = jnp.eye(stat_pair.shape[-1], dtype=jnp.float32)
    damped = stat_pair + DAMPING * identity
    frob_norm = jnp.sqrt(jnp.sum(damped * damped, axis=(1, 2), keepdims=True) + EPSILON)
    moment = damped / frob_norm
    result = jnp.broadcast_to(identity, stat_pair.shape)
    for iteration in range(ITERS):
        factor = (5.0 * identity - moment) * 0.25
        if iteration == 0:
            result = factor
        else:
            result = batched(result, factor)
        if iteration + 1 < ITERS:
            square = batched(factor, factor)
            moment = batched(square, batched(square, moment))
    return result * frob_norm ** (-0.25)


def precondition(grad_block, stat_pair):
    gram_left = lax.dot_general(
        grad_block, grad_block, (((1,), (1,)), ((), ())), preferred_element_type=jnp.float32
    )
    gram_right = lax.dot_general(
        grad_block, grad_block, (((0,), (0,)), ((), ())), preferred_element_type=jnp.float32
    )
    new_pair = BETA * stat_pair + (1.0 - BETA) * jnp.stack([gram_left, gram_right])
    root_pair = inverse_roots(new_pair)
    left_applied = jnp.dot(
        root_pair[0].astype(jnp.bfloat16), grad_block, preferred_element_type=jnp.float32
    )
    direction = jnp.dot(
        left_applied.astype(jnp.bfloat16),
        root_pair[1].astype(jnp.bfloat16),
        preferred_element_type=jnp.float32,
    )
    grad_wide = grad_block.astype(jnp.float32)
    graft_ratio = jnp.sqrt(
        (jnp.mean(grad_wide * grad_wide) + EPSILON) / (jnp.mean(direction * direction) + EPSILON)
    )
    return ((direction * graft_ratio).astype(jnp.bfloat16), new_pair)


def keep_slot(grad_block, stat_pair):
    return (jnp.zeros_like(grad_block), stat_pair)


def on_device(acts, cotangent, stats, owner_slot):
    dp_count = lax.axis_size("dp")
    my_index = lax.axis_index("dp")
    blk_size = cotangent.shape[1]
    blocks = acts.shape[1] // blk_size
    slot_count = stats.shape[1]
    piece_rows = blk_size // dp_count
    split_acts = acts.reshape(acts.shape[0], blocks, blk_size)
    my_slots = my_index * slot_count + jnp.arange(slot_count, dtype=jnp.int32)
    holds_block = owner_slot[None, :] == my_slots[:, None]
    filled = jnp.any(holds_block, axis=1)
    my_rows = lax.psum_scatter(
        jnp.einsum("twr,tc->rwc", split_acts, cotangent, preferred_element_type=jnp.float32),
        "dp",
        scatter_dimension=0,
        tiled=True,
    ).astype(jnp.bfloat16)
    slot_ids = jnp.arange(dp_count * slot_count, dtype=jnp.int32)
    selector = (owner_slot[None, :] == slot_ids[:, None]).astype(jnp.bfloat16)
    outgoing = jnp.einsum(
        "sw,rwc->src", selector, my_rows, preferred_element_type=jnp.float32
    ).astype(jnp.bfloat16)
    outgoing = outgoing.reshape(dp_count, slot_count, piece_rows, blk_size)
    arrived = lax.all_to_all(outgoing, "dp", split_axis=0, concat_axis=2, tiled=True)
    owned_grads = arrived.reshape(slot_count, blk_size, blk_size)
    slot_update, slot_stats = lax.cond(
        filled[0], precondition, keep_slot, owned_grads[0], stats[0, 0]
    )
    update_list = [slot_update]
    stat_list = [slot_stats]
    updates = jnp.stack(update_list)
    new_stats = jnp.stack(stat_list)[None]
    outgoing_rows = updates.reshape(slot_count, dp_count, piece_rows, blk_size)
    returned = lax.all_to_all(outgoing_rows, "dp", split_axis=1, concat_axis=1, tiled=True)
    grid_ids = (
        jnp.arange(slot_count, dtype=jnp.int32)[:, None]
        + slot_count * jnp.arange(dp_count, dtype=jnp.int32)[None, :]
    )
    picker = (owner_slot[:, None, None] == grid_ids[None]).astype(jnp.bfloat16)
    result = jnp.einsum(
        "wsn,snrc->wrc", picker, returned, preferred_element_type=jnp.float32
    ).astype(jnp.bfloat16)
    return (result, new_stats)


MESH = pl.DeviceIdType.MESH
LANES = 2
DEPTH = 4
CHUNKS = 4
END_ORDER = (
    "O2", "a0x", "a1=", "O1", "a2x", "O0", "O3", "A1=", "A0x", "A2x", "R10", "R11",
    "a1x", "R12", "R21", "M0x", "a3x", "A1x", "a2=", "R31", "A2=", "R20", "R13", "a3=",
    "R22", "A3x", "M1=", "R23", "R30", "A3=", "R33", "M2x", "M1x", "M2=", "R32", "M3=",
    "M3x",
)
INNER_ORDER = (
    "O3", "a0=", "a2=", "O1", "a1x", "a3x", "O2", "O0", "R01", "a0x", "a3=", "A1x",
    "R21", "A2=", "R00", "A3x", "a2x", "R03", "R31", "R20", "A0x", "R22", "R23", "R02",
    "A0=", "M2=", "M1x", "R30", "A2x", "R33", "A3=", "R32", "M0x", "M3=", "M0=", "M2x",
    "M3x",
)


def mm(former, latter):
    return jnp.dot(former, latter, preferred_element_type=jnp.float32)


def step_kernel(slot_ref, acts_ref, cot_ref, stat_ref, held_ref, new_ref,
                stage, quarters, wholes, acts_all, cot_all, total, stats, direction,
                a_send, a_recv, sib_send, sib_recv, y_send, y_recv, fwd_send, fwd_recv,
                own_send, z_send, x_send, c_recv, quarter_sem, whole_sem, cot_sem, stat_sem,
                back_send, back_recv, owner_ref, owner_sem):
    dp_count, tokens, blk = acts_all.shape
    mp_count = lax.axis_size("mp")
    part = tokens // mp_count
    chunk = tokens // CHUNKS
    me = lax.axis_index("dp")
    mine = lax.axis_index("mp")
    z, x = me // LANES, me % LANES
    half = z // (DEPTH // 2)
    sign = 1 - 2 * half
    level = half * (DEPTH - 1) + sign * z
    sibling = mine + 1 - 2 * (mine % 2)
    beside = (mine + 2) % mp_count
    across = beside + 1 - 2 * (beside % 2)

    def part_rows(m):
        return pl.ds(pl.multiple_of(m * part, part), part)

    my_rows, beside_rows = part_rows(mine), part_rows(beside)
    sibling_rows, across_rows = part_rows(sibling), part_rows(across)

    def line(i):
        return half * (DEPTH - 1) + sign * i

    def at(i, other):
        return line(i) * LANES + (1 - x if other else x)

    others = [(me + step) % dp_count for step in range(1, dp_count)]
    greeted = [(d, mine) for d in others] + [(me, m) for m in (sibling, beside, across)]
    barrier = pltpu.get_barrier_semaphore()
    for d, m in greeted:
        pl.semaphore_signal(barrier, inc=1, device_id={"dp": d, "mp": m}, device_id_type=MESH)

    cot_load = pltpu.make_async_copy(cot_ref, cot_all.at[me], cot_sem)
    cot_load.start()
    owner_load = pltpu.make_async_copy(slot_ref, owner_ref, owner_sem)
    owner_load.start()
    quarter_loads, whole_loads = [], []
    for w in range(dp_count):
        cols = pl.ds(w * blk, blk)
        quarter_loads.append(pltpu.make_async_copy(acts_ref.at[my_rows, cols], quarters.at[w], quarter_sem.at[w]))
        whole_loads.append(pltpu.make_async_copy(acts_ref.at[:, cols], wholes.at[w], whole_sem.at[w]))
    stat_load = pltpu.make_async_copy(stat_ref, stats, stat_sem)
    for load in quarter_loads + whole_loads + [stat_load]:
        load.start()

    def block_of(d):
        found = 0
        for w in range(dp_count):
            found = jnp.where(owner_ref[w] == d, w, found)
        return found

    def remote(src, dst, send, recv, d, m):
        return pltpu.make_async_remote_copy(
            src_ref=src, dst_ref=dst, send_sem=send, recv_sem=recv,
            device_id={"dp": d, "mp": m}, device_id_type=MESH)

    def arrived(ref, sem):
        pltpu.make_async_copy(ref, ref, sem).wait()

    def cot_piece(who, c):
        return cot_all.at[who, pl.ds(c * chunk, chunk)]

    def own_out(way, c, target):
        return remote(cot_piece(me, c), cot_piece(me, c), own_send.at[way, c], c_recv.at[me, c], target, mine)

    def z_out(i, to, c):
        who = at(i, False)
        return remote(cot_piece(who, c), cot_piece(who, c), z_send.at[i, c], c_recv.at[who, c], at(to, False), mine)

    def x_out(i, c):
        who = at(i, False)
        return remote(cot_piece(who, c), cot_piece(who, c), x_send.at[i, c], c_recv.at[who, c], me + 1 - 2 * x, mine)

    def acts_out(d):
        return remote(stage.at[d], acts_all.at[me, my_rows], a_send.at[d], a_recv.at[me], d, mine)

    def side_out(s, side):
        piece = acts_all.at[s, my_rows]
        return remote(piece, piece, (sib_send, y_send, fwd_send)[side].at[s], (sib_recv, y_recv, fwd_recv)[side].at[s],
                      me, (sibling, beside, across)[side])

    def own_outs(lev, c):
        copies = [own_out(0, c, at(lev + 1, False))]
        if lev > 0:
            copies.append(own_out(1, c, at(lev - 1, False)))
        return copies + [own_out(2, c, me + 1 - 2 * x)]

    def relays(lev, i, c):
        copies = [x_out(i, c)]
        if lev > 0:
            copies.append(z_out(i, lev + 1 if i < lev else lev - 1, c))
        return copies

    def by_level(act):
        for lev in range(DEPTH // 2):
            @pl.when(level == lev)
            def _(lev=lev):
                act(lev)

    def start(copies):
        for copy in copies:
            copy.start()

    def handle(word, lev):
        kind, i, which = word[0], int(word[1]), word[2:]
        if kind == "O":
            start(own_outs(lev, i))
        elif kind == "R":
            who = at(i, False)
            arrived(cot_piece(who, int(which)), c_recv.at[who, int(which)])
            start(relays(lev, i, int(which)))
        else:
            s = at(i, which == "x")
            if kind == "a":
                start([acts_out(s)])
            elif kind == "A":
                arrived(acts_all.at[s, my_rows], a_recv.at[s])
                start([side_out(s, side) for side in (1, 2, 0)])
            else:
                arrived(acts_all.at[s, sibling_rows], sib_recv.at[s])
                arrived(acts_all.at[s, beside_rows], y_recv.at[s])
                arrived(acts_all.at[s, across_rows], fwd_recv.at[s])
                if which == "x":
                    for c in range(CHUNKS):
                        arrived(cot_piece(s, c), c_recv.at[s, c])

    def parts_of(order):
        head = next(n for n, word in enumerate(order) if word[0] != "O")
        wait = next(n for n, word in enumerate(order) if word[0] in "RAM")
        found, now = [order[:head], order[head:wait]], []
        for word in order[wait:]:
            now.append(word)
            if word[0] == "M":
                found.append(now)
                now = []
        return found

    plans = [parts_of(END_ORDER), parts_of(INNER_ORDER)]

    def run_part(n):
        by_level(lambda lev: [handle(word, lev) for word in plans[lev][n]])

    def blend(end, inner):
        return end + (inner - end) * level

    def term_of(n):
        words = [plan[n][-1] for plan in plans]
        place = blend(*[int(word[1]) for word in words])
        other = blend(*[int(word[2] == "x") for word in words])
        return line(place) * LANES + x + (1 - 2 * x) * other

    def product(s):
        return lax.dot_general(acts_all[s], cot_all[s], (((0,), (0,)), ((), ())),
                               preferred_element_type=jnp.float32)

    cot_load.wait()
    pl.semaphore_wait(barrier, len(greeted))
    run_part(0)
    for load in quarter_loads + [owner_load]:
        load.wait()
    for d in range(dp_count):
        stage[d] = quarters[block_of(d)]
    run_part(1)
    for load in whole_loads:
        load.wait()
    acts_all[me] = wholes[block_of(me)]
    total[...] = product(me)
    for n in range(2, dp_count + 1):
        run_part(n)
        total[...] = total[...] + product(term_of(n))

    grad = total[...].astype(jnp.bfloat16)
    stat_load.wait()
    direction[...] = precondition_block(grad, stats, new_ref)

    def rows_of(d):
        return pl.ds(pl.multiple_of(d * held_ref.shape[1], held_ref.shape[1]), held_ref.shape[1])

    copies = []
    for step in sorted(range(1, dp_count), key=lambda step: -min(step, dp_count - step)):
        d = (me + step) % dp_count
        copies.append(remote(direction.at[rows_of(d)], held_ref.at[me], back_send.at[d], back_recv.at[me], d, mine))
        copies[-1].start()
    held_ref[me] = direction[rows_of(me)]

    def sent(lev):
        for c in range(CHUNKS):
            for copy in own_outs(lev, c) + [copy for i in range(DEPTH) if i != lev for copy in relays(lev, i, c)]:
                copy.wait_send()

    by_level(sent)
    for s in others:
        acts_out(s).wait_send()
        for side in range(3):
            side_out(s, side).wait_send()
    for d in others:
        arrived(held_ref.at[d], back_recv.at[d])
    for copy in copies:
        copy.wait_send()


def precondition_block(grad, stat_ref, new_ref):
    low = jnp.bfloat16
    blk = grad.shape[0]
    row = lax.broadcasted_iota(jnp.int32, (blk, blk), 0)
    col = lax.broadcasted_iota(jnp.int32, (blk, blk), 1)
    diagonal = row == col
    grams = [
        lax.dot_general(grad, grad, (((1,), (1,)), ((), ())), preferred_element_type=jnp.float32),
        lax.dot_general(grad, grad, (((0,), (0,)), ((), ())), preferred_element_type=jnp.float32),
    ]
    moments, results, scales = [], [None, None], []
    for side in range(2):
        fresh = BETA * stat_ref[side] + (1.0 - BETA) * grams[side]
        new_ref[side] = fresh
        damped = fresh + jnp.where(diagonal, DAMPING, 0.0)
        frob = jnp.sqrt(jnp.sum(damped * damped, axis=(0, 1), keepdims=True) + EPSILON)
        scales.append(lax.rsqrt(jnp.sqrt(frob)))
        moments.append(damped * (1.0 / frob))
    for iteration in range(ITERS):
        factors = [(jnp.where(diagonal, 5.0, 0.0) - moments[side]) * 0.25 for side in range(2)]
        lows = [factors[side].astype(low) for side in range(2)]
        if iteration + 1 < ITERS:
            squares = [mm(lows[side], lows[side]).astype(low) for side in range(2)]
            inner = [mm(squares[side], moments[side].astype(low)).astype(low) for side in range(2)]
            moments = [mm(squares[side], inner[side]) for side in range(2)]
        for side in range(2):
            results[side] = factors[side] if iteration == 0 else mm(results[side].astype(low), lows[side])
    roots = [(results[side] * scales[side]).astype(low) for side in range(2)]
    aimed = mm(mm(roots[0], grad).astype(low), roots[1])
    wide = grad.astype(jnp.float32)
    count = blk * blk
    power = jnp.sum(wide * wide, axis=(0, 1), keepdims=True) / count + EPSILON
    reached = jnp.sum(aimed * aimed, axis=(0, 1), keepdims=True) / count + EPSILON
    return (aimed * jnp.sqrt(power / reached)).astype(low)


def owned_step(owner_slot, acts, cotangent, stat_pair, dp_count, mp_count):
    tokens, blk = cotangent.shape
    low, dma = jnp.bfloat16, pltpu.SemaphoreType.DMA
    vmem, hbm = pl.BlockSpec(memory_space=pltpu.VMEM), pl.BlockSpec(memory_space=pltpu.HBM)
    return pl.pallas_call(
        step_kernel,
        name="owned_step",
        out_shape=(jax.ShapeDtypeStruct((dp_count, blk // dp_count, blk), low),
                   jax.ShapeDtypeStruct(stat_pair.shape, jnp.float32)),
        in_specs=[hbm, hbm, hbm, hbm],
        out_specs=(vmem, vmem),
        scratch_shapes=[
            pltpu.VMEM((dp_count, tokens // mp_count, blk), low),
            pltpu.VMEM((dp_count, tokens // mp_count, blk), low),
            pltpu.VMEM((dp_count, tokens, blk), low),
            pltpu.VMEM((dp_count, tokens, blk), low),
            pltpu.VMEM((dp_count, tokens, blk), low),
            pltpu.VMEM((blk, blk), jnp.float32),
            pltpu.VMEM(stat_pair.shape, jnp.float32),
            pltpu.VMEM((blk, blk), low),
        ] + [dma((dp_count,))] * 8 + [dma((3, CHUNKS)), dma((DEPTH, CHUNKS)), dma((DEPTH, CHUNKS)),
                                     dma((dp_count, CHUNKS)), dma((dp_count,)), dma((dp_count,)), dma, dma,
                                     dma((dp_count,)), dma((dp_count,)),
                                     pltpu.SMEM(owner_slot.shape, jnp.int32), dma],
        compiler_params=pltpu.CompilerParams(collective_id=0, has_side_effects=True,
                                             vmem_limit_bytes=48 * 1024 * 1024),
    )(*[pltpu.with_memory_space_constraint(a, pltpu.HBM) for a in (owner_slot, acts, cotangent, stat_pair)])


def place_kernel(owner_ref, held_ref, pair_ref, out_ref, new_ref, sems, pair_sem):
    stats_out = pltpu.make_async_copy(pair_ref, new_ref, pair_sem)
    stats_out.start()
    copies = [pltpu.make_async_copy(held_ref.at[owner_ref[w]], out_ref.at[w], sems.at[w])
              for w in range(held_ref.shape[0])]
    for copy in copies:
        copy.start()
    for copy in copies + [stats_out]:
        copy.wait()


def place_rows(owner_slot, held, new_pair):
    vmem, hbm = pl.BlockSpec(memory_space=pltpu.VMEM), pl.BlockSpec(memory_space=pltpu.HBM)
    return pl.pallas_call(
        place_kernel,
        name="place_rows",
        out_shape=(jax.ShapeDtypeStruct(held.shape, held.dtype),
                   jax.ShapeDtypeStruct(new_pair.shape, new_pair.dtype)),
        in_specs=[pl.BlockSpec(memory_space=pltpu.SMEM), vmem, vmem],
        out_specs=(hbm, hbm),
        scratch_shapes=[pltpu.SemaphoreType.DMA((held.shape[0],)), pltpu.SemaphoreType.DMA],
        compiler_params=pltpu.CompilerParams(vmem_limit_bytes=4 * 1024 * 1024),
    )(owner_slot, held, new_pair)


def full_house(acts, cotangent, stats, owner_slot):
    dp_count, mp_count = lax.axis_size("dp"), lax.axis_size("mp")
    held, new_pair = owned_step(owner_slot, acts, cotangent, stats[0, 0], dp_count, mp_count)
    update, new_pair = place_rows(owner_slot, held, new_pair)
    return update, new_pair[None, None]


def device_body(acts, cotangent, stats, owner_slot):
    dp_count, mp_count = lax.axis_size("dp"), lax.axis_size("mp")
    blk = cotangent.shape[1]
    every_slot_filled = stats.shape[1] == 1 and acts.shape[1] == dp_count * blk
    if every_slot_filled and mp_count == 4 and dp_count == LANES * DEPTH:
        return full_house(acts, cotangent, stats, owner_slot)
    return on_device(acts, cotangent, stats, owner_slot)


def solution(mesh):
    return jax.shard_map(
        device_body,
        mesh=mesh,
        in_specs=(P("dp", None), P("dp", "mp"), P("mp", "dp", None, None, None), P()),
        out_specs=(P(None, "dp", "mp"), P("mp", "dp", None, None, None)),
        check_vma=False,
    )
```

```python
import jax
import jax.numpy as jnp
from jax import lax
from jax.experimental import pallas as pl
from jax.experimental.pallas import tpu as pltpu
from jax.sharding import PartitionSpec as P

ITERS = 5


BETA = 0.9
DAMPING = 0.001
EPSILON = 1e-06


def batched(former, latter):
    return jnp.einsum(
        "kij,kjl->kil",
        former.astype(jnp.bfloat16),
        latter.astype(jnp.bfloat16),
        preferred_element_type=jnp.float32,
    )


def inverse_roots(stat_pair):
    identity = jnp.eye(stat_pair.shape[-1], dtype=jnp.float32)
    damped = stat_pair + DAMPING * identity
    frob_norm = jnp.sqrt(jnp.sum(damped * damped, axis=(1, 2), keepdims=True) + EPSILON)
    moment = damped / frob_norm
    result = jnp.broadcast_to(identity, stat_pair.shape)
    for iteration in range(ITERS):
        factor = (5.0 * identity - moment) * 0.25
        if iteration == 0:
            result = factor
        else:
            result = batched(result, factor)
        if iteration + 1 < ITERS:
            square = batched(factor, factor)
            moment = batched(square, batched(square, moment))
    return result * frob_norm ** (-0.25)


def precondition(grad_block, stat_pair):
    gram_left = lax.dot_general(
        grad_block, grad_block, (((1,), (1,)), ((), ())), preferred_element_type=jnp.float32
    )
    gram_right = lax.dot_general(
        grad_block, grad_block, (((0,), (0,)), ((), ())), preferred_element_type=jnp.float32
    )
    new_pair = BETA * stat_pair + (1.0 - BETA) * jnp.stack([gram_left, gram_right])
    root_pair = inverse_roots(new_pair)
    left_applied = jnp.dot(
        root_pair[0].astype(jnp.bfloat16), grad_block, preferred_element_type=jnp.float32
    )
    direction = jnp.dot(
        left_applied.astype(jnp.bfloat16),
        root_pair[1].astype(jnp.bfloat16),
        preferred_element_type=jnp.float32,
    )
    grad_wide = grad_block.astype(jnp.float32)
    graft_ratio = jnp.sqrt(
        (jnp.mean(grad_wide * grad_wide) + EPSILON) / (jnp.mean(direction * direction) + EPSILON)
    )
    return ((direction * graft_ratio).astype(jnp.bfloat16), new_pair)


def keep_slot(grad_block, stat_pair):
    return (jnp.zeros_like(grad_block), stat_pair)


def on_device(acts, cotangent, stats, owner_slot):
    dp_count = lax.axis_size("dp")
    my_index = lax.axis_index("dp")
    blk_size = cotangent.shape[1]
    blocks = acts.shape[1] // blk_size
    slot_count = stats.shape[1]
    piece_rows = blk_size // dp_count
    split_acts = acts.reshape(acts.shape[0], blocks, blk_size)
    my_slots = my_index * slot_count + jnp.arange(slot_count, dtype=jnp.int32)
    holds_block = owner_slot[None, :] == my_slots[:, None]
    filled = jnp.any(holds_block, axis=1)
    my_rows = lax.psum_scatter(
        jnp.einsum("twr,tc->rwc", split_acts, cotangent, preferred_element_type=jnp.float32),
        "dp",
        scatter_dimension=0,
        tiled=True,
    ).astype(jnp.bfloat16)
    slot_ids = jnp.arange(dp_count * slot_count, dtype=jnp.int32)
    selector = (owner_slot[None, :] == slot_ids[:, None]).astype(jnp.bfloat16)
    outgoing = jnp.einsum(
        "sw,rwc->src", selector, my_rows, preferred_element_type=jnp.float32
    ).astype(jnp.bfloat16)
    outgoing = outgoing.reshape(dp_count, slot_count, piece_rows, blk_size)
    arrived = lax.all_to_all(outgoing, "dp", split_axis=0, concat_axis=2, tiled=True)
    owned_grads = arrived.reshape(slot_count, blk_size, blk_size)
    slot_update, slot_stats = lax.cond(
        filled[0], precondition, keep_slot, owned_grads[0], stats[0, 0]
    )
    update_list = [slot_update]
    stat_list = [slot_stats]
    updates = jnp.stack(update_list)
    new_stats = jnp.stack(stat_list)[None]
    outgoing_rows = updates.reshape(slot_count, dp_count, piece_rows, blk_size)
    returned = lax.all_to_all(outgoing_rows, "dp", split_axis=1, concat_axis=1, tiled=True)
    grid_ids = (
        jnp.arange(slot_count, dtype=jnp.int32)[:, None]
        + slot_count * jnp.arange(dp_count, dtype=jnp.int32)[None, :]
    )
    picker = (owner_slot[:, None, None] == grid_ids[None]).astype(jnp.bfloat16)
    result = jnp.einsum(
        "wsn,snrc->wrc", picker, returned, preferred_element_type=jnp.float32
    ).astype(jnp.bfloat16)
    return (result, new_stats)


MESH = pl.DeviceIdType.MESH
LANES = 2
DEPTH = 4
CHUNKS = 4
END_ORDER = (
    "O2", "a0x", "a1=", "O1", "a2x", "O0", "O3", "A1=", "A0x", "A2x", "R10", "R11",
    "a1x", "R12", "R21", "M0x", "a3x", "A1x", "a2=", "R31", "A2=", "R20", "R13", "a3=",
    "R22", "A3x", "M1=", "R23", "R30", "A3=", "R33", "M2x", "M1x", "M2=", "R32", "M3=",
    "M3x",
)
INNER_ORDER = (
    "O3", "a0=", "a2=", "O1", "a1x", "a3x", "O2", "O0", "R01", "a0x", "a3=", "A1x",
    "R21", "A2=", "R00", "A3x", "a2x", "R03", "R31", "R20", "A0x", "R22", "R23", "R02",
    "A0=", "M2=", "M1x", "R30", "A2x", "R33", "A3=", "R32", "M0x", "M3=", "M0=", "M2x",
    "M3x",
)


BACK_ORDER = ((3, 3), (2, 0), (1, 2), (0, 1))


def mm(former, latter):
    return jnp.dot(former, latter, preferred_element_type=jnp.float32)


def step_kernel(slot_ref, acts_ref, cot_ref, stat_ref, held_ref, new_ref,
                stage, quarters, wholes, acts_all, cot_all, total, stats, direction, left_root,
                a_send, a_recv, sib_send, sib_recv, y_send, y_recv, fwd_send, fwd_recv,
                own_send, z_send, x_send, c_recv, quarter_sem, whole_sem, cot_sem, stat_sem,
                back_send, back_recv, owner_ref, owner_sem):
    dp_count, tokens, blk = acts_all.shape
    mp_count = lax.axis_size("mp")
    part = tokens // mp_count
    chunk = tokens // CHUNKS
    me = lax.axis_index("dp")
    mine = lax.axis_index("mp")
    z, x = me // LANES, me % LANES
    half = z // (DEPTH // 2)
    sign = 1 - 2 * half
    level = half * (DEPTH - 1) + sign * z
    sibling = mine + 1 - 2 * (mine % 2)
    beside = (mine + 2) % mp_count
    across = beside + 1 - 2 * (beside % 2)

    def part_rows(m):
        return pl.ds(pl.multiple_of(m * part, part), part)

    my_rows, beside_rows = part_rows(mine), part_rows(beside)
    sibling_rows, across_rows = part_rows(sibling), part_rows(across)

    def line(i):
        return half * (DEPTH - 1) + sign * i

    def at(i, other):
        return line(i) * LANES + (1 - x if other else x)

    others = [(me + step) % dp_count for step in range(1, dp_count)]
    greeted = [(d, mine) for d in others] + [(me, m) for m in (sibling, beside, across)]
    barrier = pltpu.get_barrier_semaphore()
    for d, m in greeted:
        pl.semaphore_signal(barrier, inc=1, device_id={"dp": d, "mp": m}, device_id_type=MESH)

    cot_load = pltpu.make_async_copy(cot_ref, cot_all.at[me], cot_sem)
    cot_load.start()
    owner_load = pltpu.make_async_copy(slot_ref, owner_ref, owner_sem)
    owner_load.start()
    quarter_loads, whole_loads = [], []
    for w in range(dp_count):
        cols = pl.ds(w * blk, blk)
        quarter_loads.append(pltpu.make_async_copy(acts_ref.at[my_rows, cols], quarters.at[w], quarter_sem.at[w]))
        whole_loads.append(pltpu.make_async_copy(acts_ref.at[:, cols], wholes.at[w], whole_sem.at[w]))
    stat_load = pltpu.make_async_copy(stat_ref, stats, stat_sem)
    for load in quarter_loads + whole_loads + [stat_load]:
        load.start()

    def block_of(d):
        found = 0
        for w in range(dp_count):
            found = jnp.where(owner_ref[w] == d, w, found)
        return found

    def remote(src, dst, send, recv, d, m):
        return pltpu.make_async_remote_copy(
            src_ref=src, dst_ref=dst, send_sem=send, recv_sem=recv,
            device_id={"dp": d, "mp": m}, device_id_type=MESH)

    def arrived(ref, sem):
        pltpu.make_async_copy(ref, ref, sem).wait()

    def cot_piece(who, c):
        return cot_all.at[who, pl.ds(c * chunk, chunk)]

    def own_out(way, c, target):
        return remote(cot_piece(me, c), cot_piece(me, c), own_send.at[way, c], c_recv.at[me, c], target, mine)

    def z_out(i, to, c):
        who = at(i, False)
        return remote(cot_piece(who, c), cot_piece(who, c), z_send.at[i, c], c_recv.at[who, c], at(to, False), mine)

    def x_out(i, c):
        who = at(i, False)
        return remote(cot_piece(who, c), cot_piece(who, c), x_send.at[i, c], c_recv.at[who, c], me + 1 - 2 * x, mine)

    def acts_out(d):
        return remote(stage.at[d], acts_all.at[me, my_rows], a_send.at[d], a_recv.at[me], d, mine)

    def side_out(s, side):
        piece = acts_all.at[s, my_rows]
        return remote(piece, piece, (sib_send, y_send, fwd_send)[side].at[s], (sib_recv, y_recv, fwd_recv)[side].at[s],
                      me, (sibling, beside, across)[side])

    def own_outs(lev, c):
        copies = [own_out(0, c, at(lev + 1, False))]
        if lev > 0:
            copies.append(own_out(1, c, at(lev - 1, False)))
        return copies + [own_out(2, c, me + 1 - 2 * x)]

    def relays(lev, i, c):
        copies = [x_out(i, c)]
        if lev > 0:
            copies.append(z_out(i, lev + 1 if i < lev else lev - 1, c))
        return copies

    def by_level(act):
        for lev in range(DEPTH // 2):
            @pl.when(level == lev)
            def _(lev=lev):
                act(lev)

    def start(copies):
        for copy in copies:
            copy.start()

    def handle(word, lev):
        kind, i, which = word[0], int(word[1]), word[2:]
        if kind == "O":
            start(own_outs(lev, i))
        elif kind == "R":
            who = at(i, False)
            arrived(cot_piece(who, int(which)), c_recv.at[who, int(which)])
            start(relays(lev, i, int(which)))
        else:
            s = at(i, which == "x")
            if kind == "a":
                start([acts_out(s)])
            elif kind == "A":
                arrived(acts_all.at[s, my_rows], a_recv.at[s])
                start([side_out(s, side) for side in (1, 2, 0)])
            else:
                arrived(acts_all.at[s, sibling_rows], sib_recv.at[s])
                arrived(acts_all.at[s, beside_rows], y_recv.at[s])
                arrived(acts_all.at[s, across_rows], fwd_recv.at[s])
                if which == "x":
                    for c in range(CHUNKS):
                        arrived(cot_piece(s, c), c_recv.at[s, c])

    def parts_of(order):
        head = next(n for n, word in enumerate(order) if word[0] != "O")
        wait = next(n for n, word in enumerate(order) if word[0] in "RAM")
        found, now = [order[:head], order[head:wait]], []
        for word in order[wait:]:
            now.append(word)
            if word[0] == "M":
                found.append(now)
                now = []
        return found

    plans = [parts_of(END_ORDER), parts_of(INNER_ORDER)]

    def run_part(n):
        by_level(lambda lev: [handle(word, lev) for word in plans[lev][n]])

    def blend(end, inner):
        return end + (inner - end) * level

    def term_of(n):
        words = [plan[n][-1] for plan in plans]
        place = blend(*[int(word[1]) for word in words])
        other = blend(*[int(word[2] == "x") for word in words])
        return line(place) * LANES + x + (1 - 2 * x) * other

    def product(s):
        return lax.dot_general(acts_all[s], cot_all[s], (((0,), (0,)), ((), ())),
                               preferred_element_type=jnp.float32)

    cot_load.wait()
    pl.semaphore_wait(barrier, len(greeted))
    run_part(0)
    for load in quarter_loads + [owner_load]:
        load.wait()
    for d in range(dp_count):
        stage[d] = quarters[block_of(d)]
    run_part(1)
    for load in whole_loads:
        load.wait()
    acts_all[me] = wholes[block_of(me)]
    total[...] = product(me)
    for n in range(2, dp_count + 1):
        run_part(n)
        total[...] = total[...] + product(term_of(n))

    grad = total[...].astype(jnp.bfloat16)
    stat_load.wait()
    left_root[...], right_root = roots_of(grad, stats, new_ref)
    piece = held_ref.shape[1]
    wide = grad.astype(jnp.float32)
    power, reached = jnp.sum(wide * wide, axis=(0, 1), keepdims=True), 0.0

    def rows_of(d, count=1):
        return pl.ds(pl.multiple_of(d * piece, piece), count * piece)

    planes = [line(blend(*pair)) for pair in BACK_ORDER]
    aims = []
    for plane in planes:
        aims.append(mm(mm(left_root[rows_of(plane * LANES, LANES)], grad).astype(jnp.bfloat16), right_root))
        reached = reached + jnp.sum(aims[-1] * aims[-1], axis=(0, 1), keepdims=True)
    gain = jnp.sqrt((power / wide.size + EPSILON) / (reached / wide.size + EPSILON))
    copies = []
    for n, plane in enumerate(planes):
        direction[rows_of(plane * LANES, LANES)] = (aims[n] * gain).astype(jnp.bfloat16)
        for d in ([plane * LANES + lane for lane in range(LANES)] if n + 1 < DEPTH else [me + 1 - 2 * x]):
            copies.append(remote(direction.at[rows_of(d)], held_ref.at[me], back_send.at[d], back_recv.at[me], d, mine))
            copies[-1].start()
    held_ref[me] = direction[rows_of(me)]

    def sent(lev):
        for c in range(CHUNKS):
            for copy in own_outs(lev, c) + [copy for i in range(DEPTH) if i != lev for copy in relays(lev, i, c)]:
                copy.wait_send()

    by_level(sent)
    for s in others:
        acts_out(s).wait_send()
        for side in range(3):
            side_out(s, side).wait_send()
    for d in others:
        arrived(held_ref.at[d], back_recv.at[d])
    for copy in copies:
        copy.wait_send()


def roots_of(grad, stat_ref, new_ref):
    low = jnp.bfloat16
    blk = grad.shape[0]
    half = blk // 2
    row = lax.broadcasted_iota(jnp.int32, (half, half), 0)
    col = lax.broadcasted_iota(jnp.int32, (half, half), 1)
    diagonal = row == col

    def whole(parts):
        near, cross, far = [part.astype(low) for part in parts]
        return jnp.concatenate([jnp.concatenate([near, cross], 1), jnp.concatenate([cross.T, far], 1)], 0)

    def product(former, latter):
        top = mm(former[:half], latter)
        return top[:, :half], top[:, half:], mm(former[half:], latter[:, half:])

    def gram(rows):
        def part(a, b):
            return lax.dot_general(a, b, (((1,), (1,)), ((), ())), preferred_element_type=jnp.float32)

        top = part(rows[:half], rows)
        return top[:, :half], top[:, half:], part(rows[half:], rows[half:])

    def gram_t(cols):
        def part(a, b):
            return lax.dot_general(a, b, (((0,), (0,)), ((), ())), preferred_element_type=jnp.float32)

        top = part(cols[:, :half], cols)
        return top[:, :half], top[:, half:], part(cols[:, half:], cols[:, half:])

    def total_of(parts):
        near, cross, far = [jnp.sum(part * part, axis=(0, 1), keepdims=True) for part in parts]
        return near + 2.0 * cross + far

    spots = [(slice(0, half), slice(0, half)), (slice(0, half), slice(half, blk)), (slice(half, blk), slice(half, blk))]
    moments, results, scales = [], [None, None], []
    for side, grams in enumerate((gram(grad), gram_t(grad))):
        fresh = [BETA * stat_ref[side, r, c] + (1.0 - BETA) * part for (r, c), part in zip(spots, grams)]
        for (r, c), part in zip(spots, fresh):
            new_ref[side, r, c] = part
        new_ref[side, half:, :half] = fresh[1].T
        shift = jnp.where(diagonal, DAMPING, 0.0)
        damped = [fresh[0] + shift, fresh[1], fresh[2] + shift]
        frob = jnp.sqrt(total_of(damped) + EPSILON)
        scales.append(lax.rsqrt(jnp.sqrt(frob)))
        moments.append([part * (1.0 / frob) for part in damped])
    for iteration in range(ITERS):
        five = jnp.where(diagonal, 5.0, 0.0)
        factors = [[(five - m[0]) * 0.25, m[1] * -0.25, (five - m[2]) * 0.25] for m in moments]
        lows = [whole(factor) for factor in factors]
        if iteration + 1 < ITERS:
            squares = [whole(product(lows[side], lows[side])) for side in range(2)]
            inner = [whole(product(squares[side], whole(moments[side]))) for side in range(2)]
            moments = [product(squares[side], inner[side]) for side in range(2)]
        for side in range(2):
            results[side] = factors[side] if iteration == 0 else product(whole(results[side]), lows[side])
    return [whole([part * scales[side] for part in results[side]]) for side in range(2)]


def owned_step(owner_slot, acts, cotangent, stat_pair, dp_count, mp_count):
    tokens, blk = cotangent.shape
    low, dma = jnp.bfloat16, pltpu.SemaphoreType.DMA
    vmem, hbm = pl.BlockSpec(memory_space=pltpu.VMEM), pl.BlockSpec(memory_space=pltpu.HBM)
    return pl.pallas_call(
        step_kernel,
        name="owned_step",
        out_shape=(jax.ShapeDtypeStruct((dp_count, blk // dp_count, blk), low),
                   jax.ShapeDtypeStruct(stat_pair.shape, jnp.float32)),
        in_specs=[hbm, hbm, hbm, hbm],
        out_specs=(vmem, vmem),
        scratch_shapes=[
            pltpu.VMEM((dp_count, tokens // mp_count, blk), low),
            pltpu.VMEM((dp_count, tokens // mp_count, blk), low),
            pltpu.VMEM((dp_count, tokens, blk), low),
            pltpu.VMEM((dp_count, tokens, blk), low),
            pltpu.VMEM((dp_count, tokens, blk), low),
            pltpu.VMEM((blk, blk), jnp.float32),
            pltpu.VMEM(stat_pair.shape, jnp.float32),
            pltpu.VMEM((blk, blk), low),
            pltpu.VMEM((blk, blk), low),
        ] + [dma((dp_count,))] * 8 + [dma((3, CHUNKS)), dma((DEPTH, CHUNKS)), dma((DEPTH, CHUNKS)),
                                     dma((dp_count, CHUNKS)), dma((dp_count,)), dma((dp_count,)), dma, dma,
                                     dma((dp_count,)), dma((dp_count,)),
                                     pltpu.SMEM(owner_slot.shape, jnp.int32), dma],
        compiler_params=pltpu.CompilerParams(collective_id=0, has_side_effects=True,
                                             vmem_limit_bytes=48 * 1024 * 1024),
    )(*[pltpu.with_memory_space_constraint(a, pltpu.HBM) for a in (owner_slot, acts, cotangent, stat_pair)])


def place_kernel(owner_ref, held_ref, pair_ref, out_ref, new_ref, sems, pair_sem):
    stats_out = pltpu.make_async_copy(pair_ref, new_ref, pair_sem)
    stats_out.start()
    copies = [pltpu.make_async_copy(held_ref.at[owner_ref[w]], out_ref.at[w], sems.at[w])
              for w in range(held_ref.shape[0])]
    for copy in copies:
        copy.start()
    for copy in copies + [stats_out]:
        copy.wait()


def place_rows(owner_slot, held, new_pair):
    vmem, hbm = pl.BlockSpec(memory_space=pltpu.VMEM), pl.BlockSpec(memory_space=pltpu.HBM)
    return pl.pallas_call(
        place_kernel,
        name="place_rows",
        out_shape=(jax.ShapeDtypeStruct(held.shape, held.dtype),
                   jax.ShapeDtypeStruct(new_pair.shape, new_pair.dtype)),
        in_specs=[pl.BlockSpec(memory_space=pltpu.SMEM), vmem, vmem],
        out_specs=(hbm, hbm),
        scratch_shapes=[pltpu.SemaphoreType.DMA((held.shape[0],)), pltpu.SemaphoreType.DMA],
        compiler_params=pltpu.CompilerParams(vmem_limit_bytes=4 * 1024 * 1024),
    )(owner_slot, held, new_pair)


def full_house(acts, cotangent, stats, owner_slot):
    dp_count, mp_count = lax.axis_size("dp"), lax.axis_size("mp")
    held, new_pair = owned_step(owner_slot, acts, cotangent, stats[0, 0], dp_count, mp_count)
    update, new_pair = place_rows(owner_slot, held, new_pair)
    return update, new_pair[None, None]


def device_body(acts, cotangent, stats, owner_slot):
    dp_count, mp_count = lax.axis_size("dp"), lax.axis_size("mp")
    blk = cotangent.shape[1]
    every_slot_filled = stats.shape[1] == 1 and acts.shape[1] == dp_count * blk
    if every_slot_filled and mp_count == 4 and dp_count == LANES * DEPTH:
        return full_house(acts, cotangent, stats, owner_slot)
    return on_device(acts, cotangent, stats, owner_slot)


def solution(mesh):
    return jax.shard_map(
        device_body,
        mesh=mesh,
        in_specs=(P("dp", None), P("dp", "mp"), P("mp", "dp", None, None, None), P()),
        out_specs=(P(None, "dp", "mp"), P("mp", "dp", None, None, None)),
        check_vma=False,
    )
```

```python
import jax
import jax.numpy as jnp
from jax import lax
from jax.experimental import pallas as pl
from jax.experimental.pallas import tpu as pltpu
from jax.sharding import PartitionSpec as P

ITERS = 5


BETA = 0.9
DAMPING = 0.001
EPSILON = 1e-06


def batched(former, latter):
    return jnp.einsum(
        "kij,kjl->kil",
        former.astype(jnp.bfloat16),
        latter.astype(jnp.bfloat16),
        preferred_element_type=jnp.float32,
    )


def inverse_roots(stat_pair):
    identity = jnp.eye(stat_pair.shape[-1], dtype=jnp.float32)
    damped = stat_pair + DAMPING * identity
    frob_norm = jnp.sqrt(jnp.sum(damped * damped, axis=(1, 2), keepdims=True) + EPSILON)
    moment = damped / frob_norm
    result = jnp.broadcast_to(identity, stat_pair.shape)
    for iteration in range(ITERS):
        factor = (5.0 * identity - moment) * 0.25
        if iteration == 0:
            result = factor
        else:
            result = batched(result, factor)
        if iteration + 1 < ITERS:
            square = batched(factor, factor)
            moment = batched(square, batched(square, moment))
    return result * frob_norm ** (-0.25)


def precondition(grad_block, stat_pair):
    gram_left = lax.dot_general(
        grad_block, grad_block, (((1,), (1,)), ((), ())), preferred_element_type=jnp.float32
    )
    gram_right = lax.dot_general(
        grad_block, grad_block, (((0,), (0,)), ((), ())), preferred_element_type=jnp.float32
    )
    new_pair = BETA * stat_pair + (1.0 - BETA) * jnp.stack([gram_left, gram_right])
    root_pair = inverse_roots(new_pair)
    left_applied = jnp.dot(
        root_pair[0].astype(jnp.bfloat16), grad_block, preferred_element_type=jnp.float32
    )
    direction = jnp.dot(
        left_applied.astype(jnp.bfloat16),
        root_pair[1].astype(jnp.bfloat16),
        preferred_element_type=jnp.float32,
    )
    grad_wide = grad_block.astype(jnp.float32)
    graft_ratio = jnp.sqrt(
        (jnp.mean(grad_wide * grad_wide) + EPSILON) / (jnp.mean(direction * direction) + EPSILON)
    )
    return ((direction * graft_ratio).astype(jnp.bfloat16), new_pair)


def keep_slot(grad_block, stat_pair):
    return (jnp.zeros_like(grad_block), stat_pair)


def on_device(acts, cotangent, stats, owner_slot):
    dp_count = lax.axis_size("dp")
    my_index = lax.axis_index("dp")
    blk_size = cotangent.shape[1]
    blocks = acts.shape[1] // blk_size
    slot_count = stats.shape[1]
    piece_rows = blk_size // dp_count
    split_acts = acts.reshape(acts.shape[0], blocks, blk_size)
    my_slots = my_index * slot_count + jnp.arange(slot_count, dtype=jnp.int32)
    holds_block = owner_slot[None, :] == my_slots[:, None]
    filled = jnp.any(holds_block, axis=1)
    my_rows = lax.psum_scatter(
        jnp.einsum("twr,tc->rwc", split_acts, cotangent, preferred_element_type=jnp.float32),
        "dp",
        scatter_dimension=0,
        tiled=True,
    ).astype(jnp.bfloat16)
    slot_ids = jnp.arange(dp_count * slot_count, dtype=jnp.int32)
    selector = (owner_slot[None, :] == slot_ids[:, None]).astype(jnp.bfloat16)
    outgoing = jnp.einsum(
        "sw,rwc->src", selector, my_rows, preferred_element_type=jnp.float32
    ).astype(jnp.bfloat16)
    outgoing = outgoing.reshape(dp_count, slot_count, piece_rows, blk_size)
    arrived = lax.all_to_all(outgoing, "dp", split_axis=0, concat_axis=2, tiled=True)
    owned_grads = arrived.reshape(slot_count, blk_size, blk_size)
    slot_update, slot_stats = lax.cond(
        filled[0], precondition, keep_slot, owned_grads[0], stats[0, 0]
    )
    update_list = [slot_update]
    stat_list = [slot_stats]
    updates = jnp.stack(update_list)
    new_stats = jnp.stack(stat_list)[None]
    outgoing_rows = updates.reshape(slot_count, dp_count, piece_rows, blk_size)
    returned = lax.all_to_all(outgoing_rows, "dp", split_axis=1, concat_axis=1, tiled=True)
    grid_ids = (
        jnp.arange(slot_count, dtype=jnp.int32)[:, None]
        + slot_count * jnp.arange(dp_count, dtype=jnp.int32)[None, :]
    )
    picker = (owner_slot[:, None, None] == grid_ids[None]).astype(jnp.bfloat16)
    result = jnp.einsum(
        "wsn,snrc->wrc", picker, returned, preferred_element_type=jnp.float32
    ).astype(jnp.bfloat16)
    return (result, new_stats)


MESH = pl.DeviceIdType.MESH
LANES = 2
DEPTH = 4
CHUNKS = 4
END_ORDER = (
    "O2", "a0x", "a1=", "O1", "a2x", "O0", "O3", "A1=", "A0x", "A2x", "R10", "R11",
    "a1x", "R12", "R21", "M0x", "a3x", "A1x", "a2=", "R31", "A2=", "R20", "R13", "a3=",
    "R22", "A3x", "M1=", "R23", "R30", "A3=", "R33", "M2x", "M1x", "M2=", "R32", "M3=",
    "M3x",
)
INNER_ORDER = (
    "O3", "a0=", "a2=", "O1", "a1x", "a3x", "O2", "O0", "R01", "a0x", "a3=", "A1x",
    "R21", "A2=", "R00", "A3x", "a2x", "R03", "R31", "R20", "A0x", "R22", "R23", "R02",
    "A0=", "M2=", "M1x", "R30", "A2x", "R33", "A3=", "R32", "M0x", "M3=", "M0=", "M2x",
    "M3x",
)


BACK_ORDER = ((3, 3), (2, 0), (1, 2), (0, 1))


def mm(former, latter):
    return jnp.dot(former, latter, preferred_element_type=jnp.float32)


def step_kernel(slot_ref, acts_ref, cot_ref, stat_ref, out_ref, new_ref,
                stage, quarters, wholes, acts_all, cot_all, total, stats, direction, left_root, held_ref,
                a_send, a_recv, sib_send, sib_recv, y_send, y_recv, fwd_send, fwd_recv,
                own_send, z_send, x_send, c_recv, quarter_sem, whole_sem, cot_sem, stat_sem,
                back_send, back_recv, owner_ref, owner_sem):
    dp_count, tokens, blk = acts_all.shape
    mp_count = lax.axis_size("mp")
    part = tokens // mp_count
    chunk = tokens // CHUNKS
    me = lax.axis_index("dp")
    mine = lax.axis_index("mp")
    z, x = me // LANES, me % LANES
    half = z // (DEPTH // 2)
    sign = 1 - 2 * half
    level = half * (DEPTH - 1) + sign * z
    sibling = mine + 1 - 2 * (mine % 2)
    beside = (mine + 2) % mp_count
    across = beside + 1 - 2 * (beside % 2)

    def part_rows(m):
        return pl.ds(pl.multiple_of(m * part, part), part)

    my_rows, beside_rows = part_rows(mine), part_rows(beside)
    sibling_rows, across_rows = part_rows(sibling), part_rows(across)

    def line(i):
        return half * (DEPTH - 1) + sign * i

    def at(i, other):
        return line(i) * LANES + (1 - x if other else x)

    others = [(me + step) % dp_count for step in range(1, dp_count)]
    greeted = [(d, mine) for d in others] + [(me, m) for m in (sibling, beside, across)]
    barrier = pltpu.get_barrier_semaphore()
    for d, m in greeted:
        pl.semaphore_signal(barrier, inc=1, device_id={"dp": d, "mp": m}, device_id_type=MESH)

    cot_load = pltpu.make_async_copy(cot_ref, cot_all.at[me], cot_sem)
    cot_load.start()
    owner_load = pltpu.make_async_copy(slot_ref, owner_ref, owner_sem)
    owner_load.start()
    quarter_loads, whole_loads = [], []
    for w in range(dp_count):
        cols = pl.ds(w * blk, blk)
        quarter_loads.append(pltpu.make_async_copy(acts_ref.at[my_rows, cols], quarters.at[w], quarter_sem.at[w]))
        whole_loads.append(pltpu.make_async_copy(acts_ref.at[:, cols], wholes.at[w], whole_sem.at[w]))
    stat_load = pltpu.make_async_copy(stat_ref, stats, stat_sem)
    for load in quarter_loads + whole_loads + [stat_load]:
        load.start()

    def block_of(d):
        found = 0
        for w in range(dp_count):
            found = jnp.where(owner_ref[w] == d, w, found)
        return found

    def remote(src, dst, send, recv, d, m):
        return pltpu.make_async_remote_copy(
            src_ref=src, dst_ref=dst, send_sem=send, recv_sem=recv,
            device_id={"dp": d, "mp": m}, device_id_type=MESH)

    def arrived(ref, sem):
        pltpu.make_async_copy(ref, ref, sem).wait()

    def cot_piece(who, c):
        return cot_all.at[who, pl.ds(c * chunk, chunk)]

    def own_out(way, c, target):
        return remote(cot_piece(me, c), cot_piece(me, c), own_send.at[way, c], c_recv.at[me, c], target, mine)

    def z_out(i, to, c):
        who = at(i, False)
        return remote(cot_piece(who, c), cot_piece(who, c), z_send.at[i, c], c_recv.at[who, c], at(to, False), mine)

    def x_out(i, c):
        who = at(i, False)
        return remote(cot_piece(who, c), cot_piece(who, c), x_send.at[i, c], c_recv.at[who, c], me + 1 - 2 * x, mine)

    def acts_out(d):
        return remote(stage.at[d], acts_all.at[me, my_rows], a_send.at[d], a_recv.at[me], d, mine)

    def side_out(s, side):
        piece = acts_all.at[s, my_rows]
        return remote(piece, piece, (sib_send, y_send, fwd_send)[side].at[s], (sib_recv, y_recv, fwd_recv)[side].at[s],
                      me, (sibling, beside, across)[side])

    def own_outs(lev, c):
        copies = [own_out(0, c, at(lev + 1, False))]
        if lev > 0:
            copies.append(own_out(1, c, at(lev - 1, False)))
        return copies + [own_out(2, c, me + 1 - 2 * x)]

    def relays(lev, i, c):
        copies = [x_out(i, c)]
        if lev > 0:
            copies.append(z_out(i, lev + 1 if i < lev else lev - 1, c))
        return copies

    def by_level(act):
        for lev in range(DEPTH // 2):
            @pl.when(level == lev)
            def _(lev=lev):
                act(lev)

    def start(copies):
        for copy in copies:
            copy.start()

    def handle(word, lev):
        kind, i, which = word[0], int(word[1]), word[2:]
        if kind == "O":
            start(own_outs(lev, i))
        elif kind == "R":
            who = at(i, False)
            arrived(cot_piece(who, int(which)), c_recv.at[who, int(which)])
            start(relays(lev, i, int(which)))
        else:
            s = at(i, which == "x")
            if kind == "a":
                start([acts_out(s)])
            elif kind == "A":
                arrived(acts_all.at[s, my_rows], a_recv.at[s])
                start([side_out(s, side) for side in (1, 2, 0)])
            else:
                arrived(acts_all.at[s, sibling_rows], sib_recv.at[s])
                arrived(acts_all.at[s, beside_rows], y_recv.at[s])
                arrived(acts_all.at[s, across_rows], fwd_recv.at[s])
                if which == "x":
                    for c in range(CHUNKS):
                        arrived(cot_piece(s, c), c_recv.at[s, c])

    def parts_of(order):
        head = next(n for n, word in enumerate(order) if word[0] != "O")
        wait = next(n for n, word in enumerate(order) if word[0] in "RAM")
        found, now = [order[:head], order[head:wait]], []
        for word in order[wait:]:
            now.append(word)
            if word[0] == "M":
                found.append(now)
                now = []
        return found

    plans = [parts_of(END_ORDER), parts_of(INNER_ORDER)]

    def run_part(n):
        by_level(lambda lev: [handle(word, lev) for word in plans[lev][n]])

    def blend(end, inner):
        return end + (inner - end) * level

    def term_of(n):
        words = [plan[n][-1] for plan in plans]
        place = blend(*[int(word[1]) for word in words])
        other = blend(*[int(word[2] == "x") for word in words])
        return line(place) * LANES + x + (1 - 2 * x) * other

    def product(s):
        return lax.dot_general(acts_all[s], cot_all[s], (((0,), (0,)), ((), ())),
                               preferred_element_type=jnp.float32)

    cot_load.wait()
    pl.semaphore_wait(barrier, len(greeted))
    run_part(0)
    for load in quarter_loads + [owner_load]:
        load.wait()
    for d in range(dp_count):
        stage[d] = quarters[block_of(d)]
    run_part(1)
    for load in whole_loads:
        load.wait()
    acts_all[me] = wholes[block_of(me)]
    total[...] = product(me)
    for n in range(2, dp_count + 1):
        run_part(n)
        total[...] = total[...] + product(term_of(n))

    grad = total[...].astype(jnp.bfloat16)
    stat_load.wait()
    left_root[...], right_root = roots_of(grad, stats, new_ref)
    piece = held_ref.shape[1]
    wide = grad.astype(jnp.float32)
    power, reached = jnp.sum(wide * wide, axis=(0, 1), keepdims=True), 0.0

    def rows_of(d, count=1):
        return pl.ds(pl.multiple_of(d * piece, piece), count * piece)

    planes = [line(blend(*pair)) for pair in BACK_ORDER]
    aims = []
    for plane in planes:
        aims.append(mm(mm(left_root[rows_of(plane * LANES, LANES)], grad).astype(jnp.bfloat16), right_root))
        reached = reached + jnp.sum(aims[-1] * aims[-1], axis=(0, 1), keepdims=True)
    gain = jnp.sqrt((power / wide.size + EPSILON) / (reached / wide.size + EPSILON))
    copies = []
    for n, plane in enumerate(planes):
        direction[rows_of(plane * LANES, LANES)] = (aims[n] * gain).astype(jnp.bfloat16)
        for d in ([plane * LANES + lane for lane in range(LANES)] if n + 1 < DEPTH else [me + 1 - 2 * x]):
            copies.append(remote(direction.at[rows_of(d)], held_ref.at[me], back_send.at[d], back_recv.at[me], d, mine))
            copies[-1].start()
    held_ref[me] = direction[rows_of(me)]

    def sent(lev):
        for c in range(CHUNKS):
            for copy in own_outs(lev, c) + [copy for i in range(DEPTH) if i != lev for copy in relays(lev, i, c)]:
                copy.wait_send()

    by_level(sent)
    for s in others:
        acts_out(s).wait_send()
        for side in range(3):
            side_out(s, side).wait_send()
    for d in others:
        arrived(held_ref.at[d], back_recv.at[d])
    for w in range(dp_count):
        out_ref[w] = held_ref[owner_ref[w]]
    for copy in copies:
        copy.wait_send()


def roots_of(grad, stat_ref, new_ref):
    low = jnp.bfloat16
    blk = grad.shape[0]
    half = blk // 2
    row = lax.broadcasted_iota(jnp.int32, (half, half), 0)
    col = lax.broadcasted_iota(jnp.int32, (half, half), 1)
    diagonal = row == col

    def whole(parts):
        near, cross, far = [part.astype(low) for part in parts]
        return jnp.concatenate([jnp.concatenate([near, cross], 1), jnp.concatenate([cross.T, far], 1)], 0)

    def product(former, latter):
        top = mm(former[:half], latter)
        return top[:, :half], top[:, half:], mm(former[half:], latter[:, half:])

    def gram(rows):
        def part(a, b):
            return lax.dot_general(a, b, (((1,), (1,)), ((), ())), preferred_element_type=jnp.float32)

        top = part(rows[:half], rows)
        return top[:, :half], top[:, half:], part(rows[half:], rows[half:])

    def gram_t(cols):
        def part(a, b):
            return lax.dot_general(a, b, (((0,), (0,)), ((), ())), preferred_element_type=jnp.float32)

        top = part(cols[:, :half], cols)
        return top[:, :half], top[:, half:], part(cols[:, half:], cols[:, half:])

    def total_of(parts):
        near, cross, far = [jnp.sum(part * part, axis=(0, 1), keepdims=True) for part in parts]
        return near + 2.0 * cross + far

    spots = [(slice(0, half), slice(0, half)), (slice(0, half), slice(half, blk)), (slice(half, blk), slice(half, blk))]
    moments, results, scales = [], [None, None], []
    for side, grams in enumerate((gram(grad), gram_t(grad))):
        fresh = [BETA * stat_ref[side, r, c] + (1.0 - BETA) * part for (r, c), part in zip(spots, grams)]
        for (r, c), part in zip(spots, fresh):
            new_ref[side, r, c] = part
        new_ref[side, half:, :half] = fresh[1].T
        shift = jnp.where(diagonal, DAMPING, 0.0)
        damped = [fresh[0] + shift, fresh[1], fresh[2] + shift]
        frob = jnp.sqrt(total_of(damped) + EPSILON)
        scales.append(lax.rsqrt(jnp.sqrt(frob)))
        moments.append([part * (1.0 / frob) for part in damped])
    for iteration in range(ITERS):
        five = jnp.where(diagonal, 5.0, 0.0)
        factors = [[(five - m[0]) * 0.25, m[1] * -0.25, (five - m[2]) * 0.25] for m in moments]
        lows = [whole(factor) for factor in factors]
        if iteration + 1 < ITERS:
            squares = [whole(product(lows[side], lows[side])) for side in range(2)]
            inner = [whole(product(squares[side], whole(moments[side]))) for side in range(2)]
            moments = [product(squares[side], inner[side]) for side in range(2)]
        for side in range(2):
            results[side] = factors[side] if iteration == 0 else product(whole(results[side]), lows[side])
    return [whole([part * scales[side] for part in results[side]]) for side in range(2)]


def owned_step(owner_slot, acts, cotangent, stat_pair, dp_count, mp_count):
    tokens, blk = cotangent.shape
    low, dma = jnp.bfloat16, pltpu.SemaphoreType.DMA
    vmem, hbm = pl.BlockSpec(memory_space=pltpu.VMEM), pl.BlockSpec(memory_space=pltpu.HBM)
    return pl.pallas_call(
        step_kernel,
        name="owned_step",
        out_shape=(jax.ShapeDtypeStruct((dp_count, blk // dp_count, blk), low),
                   jax.ShapeDtypeStruct(stat_pair.shape, jnp.float32)),
        in_specs=[hbm, hbm, hbm, hbm],
        out_specs=(vmem, vmem),
        scratch_shapes=[
            pltpu.VMEM((dp_count, tokens // mp_count, blk), low),
            pltpu.VMEM((dp_count, tokens // mp_count, blk), low),
            pltpu.VMEM((dp_count, tokens, blk), low),
            pltpu.VMEM((dp_count, tokens, blk), low),
            pltpu.VMEM((dp_count, tokens, blk), low),
            pltpu.VMEM((blk, blk), jnp.float32),
            pltpu.VMEM(stat_pair.shape, jnp.float32),
            pltpu.VMEM((blk, blk), low),
            pltpu.VMEM((blk, blk), low),
            pltpu.VMEM((dp_count, blk // dp_count, blk), low),
        ] + [dma((dp_count,))] * 8 + [dma((3, CHUNKS)), dma((DEPTH, CHUNKS)), dma((DEPTH, CHUNKS)),
                                     dma((dp_count, CHUNKS)), dma((dp_count,)), dma((dp_count,)), dma, dma,
                                     dma((dp_count,)), dma((dp_count,)),
                                     pltpu.SMEM(owner_slot.shape, jnp.int32), dma],
        compiler_params=pltpu.CompilerParams(collective_id=0, has_side_effects=True,
                                             vmem_limit_bytes=48 * 1024 * 1024),
    )(*[pltpu.with_memory_space_constraint(a, pltpu.HBM) for a in (owner_slot, acts, cotangent, stat_pair)])


def place_kernel(rows_ref, pair_ref, out_ref, new_ref, rows_sem, pair_sem):
    copies = [pltpu.make_async_copy(pair_ref, new_ref, pair_sem), pltpu.make_async_copy(rows_ref, out_ref, rows_sem)]
    for copy in copies:
        copy.start()
    for copy in copies:
        copy.wait()


def place(rows, new_pair):
    vmem, hbm = pl.BlockSpec(memory_space=pltpu.VMEM), pl.BlockSpec(memory_space=pltpu.HBM)
    return pl.pallas_call(
        place_kernel,
        name="place",
        out_shape=(jax.ShapeDtypeStruct(rows.shape, rows.dtype),
                   jax.ShapeDtypeStruct(new_pair.shape, new_pair.dtype)),
        in_specs=[vmem, vmem],
        out_specs=(hbm, hbm),
        scratch_shapes=[pltpu.SemaphoreType.DMA, pltpu.SemaphoreType.DMA],
        compiler_params=pltpu.CompilerParams(vmem_limit_bytes=4 * 1024 * 1024),
    )(rows, new_pair)


def full_house(acts, cotangent, stats, owner_slot):
    dp_count, mp_count = lax.axis_size("dp"), lax.axis_size("mp")
    rows, new_pair = owned_step(owner_slot, acts, cotangent, stats[0, 0], dp_count, mp_count)
    update, new_pair = place(rows, new_pair)
    return update, new_pair[None, None]


def device_body(acts, cotangent, stats, owner_slot):
    dp_count, mp_count = lax.axis_size("dp"), lax.axis_size("mp")
    blk = cotangent.shape[1]
    every_slot_filled = stats.shape[1] == 1 and acts.shape[1] == dp_count * blk
    if every_slot_filled and mp_count == 4 and dp_count == LANES * DEPTH:
        return full_house(acts, cotangent, stats, owner_slot)
    return on_device(acts, cotangent, stats, owner_slot)


def solution(mesh):
    return jax.shard_map(
        device_body,
        mesh=mesh,
        in_specs=(P("dp", None), P("dp", "mp"), P("mp", "dp", None, None, None), P()),
        out_specs=(P(None, "dp", "mp"), P("mp", "dp", None, None, None)),
        check_vma=False,
    )
```

```python
import jax
import jax.numpy as jnp
from jax import lax
from jax.experimental import pallas as pl
from jax.experimental.pallas import tpu as pltpu
from jax.sharding import PartitionSpec as P

ITERS = 5


BETA = 0.9
DAMPING = 0.001
EPSILON = 1e-06


def batched(former, latter):
    return jnp.einsum(
        "kij,kjl->kil",
        former.astype(jnp.bfloat16),
        latter.astype(jnp.bfloat16),
        preferred_element_type=jnp.float32,
    )


def inverse_roots(stat_pair):
    identity = jnp.eye(stat_pair.shape[-1], dtype=jnp.float32)
    damped = stat_pair + DAMPING * identity
    frob_norm = jnp.sqrt(jnp.sum(damped * damped, axis=(1, 2), keepdims=True) + EPSILON)
    moment = damped / frob_norm
    result = jnp.broadcast_to(identity, stat_pair.shape)
    for iteration in range(ITERS):
        factor = (5.0 * identity - moment) * 0.25
        if iteration == 0:
            result = factor
        else:
            result = batched(result, factor)
        if iteration + 1 < ITERS:
            square = batched(factor, factor)
            moment = batched(square, batched(square, moment))
    return result * frob_norm ** (-0.25)


def precondition(grad_block, stat_pair):
    gram_left = lax.dot_general(
        grad_block, grad_block, (((1,), (1,)), ((), ())), preferred_element_type=jnp.float32
    )
    gram_right = lax.dot_general(
        grad_block, grad_block, (((0,), (0,)), ((), ())), preferred_element_type=jnp.float32
    )
    new_pair = BETA * stat_pair + (1.0 - BETA) * jnp.stack([gram_left, gram_right])
    root_pair = inverse_roots(new_pair)
    left_applied = jnp.dot(
        root_pair[0].astype(jnp.bfloat16), grad_block, preferred_element_type=jnp.float32
    )
    direction = jnp.dot(
        left_applied.astype(jnp.bfloat16),
        root_pair[1].astype(jnp.bfloat16),
        preferred_element_type=jnp.float32,
    )
    grad_wide = grad_block.astype(jnp.float32)
    graft_ratio = jnp.sqrt(
        (jnp.mean(grad_wide * grad_wide) + EPSILON) / (jnp.mean(direction * direction) + EPSILON)
    )
    return ((direction * graft_ratio).astype(jnp.bfloat16), new_pair)


def keep_slot(grad_block, stat_pair):
    return (jnp.zeros_like(grad_block), stat_pair)


def on_device(acts, cotangent, stats, owner_slot):
    dp_count = lax.axis_size("dp")
    my_index = lax.axis_index("dp")
    blk_size = cotangent.shape[1]
    blocks = acts.shape[1] // blk_size
    slot_count = stats.shape[1]
    piece_rows = blk_size // dp_count
    split_acts = acts.reshape(acts.shape[0], blocks, blk_size)
    my_slots = my_index * slot_count + jnp.arange(slot_count, dtype=jnp.int32)
    holds_block = owner_slot[None, :] == my_slots[:, None]
    filled = jnp.any(holds_block, axis=1)
    my_rows = lax.psum_scatter(
        jnp.einsum("twr,tc->rwc", split_acts, cotangent, preferred_element_type=jnp.float32),
        "dp",
        scatter_dimension=0,
        tiled=True,
    ).astype(jnp.bfloat16)
    slot_ids = jnp.arange(dp_count * slot_count, dtype=jnp.int32)
    selector = (owner_slot[None, :] == slot_ids[:, None]).astype(jnp.bfloat16)
    outgoing = jnp.einsum(
        "sw,rwc->src", selector, my_rows, preferred_element_type=jnp.float32
    ).astype(jnp.bfloat16)
    outgoing = outgoing.reshape(dp_count, slot_count, piece_rows, blk_size)
    arrived = lax.all_to_all(outgoing, "dp", split_axis=0, concat_axis=2, tiled=True)
    owned_grads = arrived.reshape(slot_count, blk_size, blk_size)
    slot_update, slot_stats = lax.cond(
        filled[0], precondition, keep_slot, owned_grads[0], stats[0, 0]
    )
    update_list = [slot_update]
    stat_list = [slot_stats]
    updates = jnp.stack(update_list)
    new_stats = jnp.stack(stat_list)[None]
    outgoing_rows = updates.reshape(slot_count, dp_count, piece_rows, blk_size)
    returned = lax.all_to_all(outgoing_rows, "dp", split_axis=1, concat_axis=1, tiled=True)
    grid_ids = (
        jnp.arange(slot_count, dtype=jnp.int32)[:, None]
        + slot_count * jnp.arange(dp_count, dtype=jnp.int32)[None, :]
    )
    picker = (owner_slot[:, None, None] == grid_ids[None]).astype(jnp.bfloat16)
    result = jnp.einsum(
        "wsn,snrc->wrc", picker, returned, preferred_element_type=jnp.float32
    ).astype(jnp.bfloat16)
    return (result, new_stats)


MESH = pl.DeviceIdType.MESH
LANES = 2
DEPTH = 4
CHUNKS = 4
END_ORDER = (
    "O2", "a0x", "a1=", "O1", "a2x", "O0", "O3", "A1=", "A0x", "A2x", "R10", "R11",
    "a1x", "R12", "R21", "M0x", "a3x", "A1x", "a2=", "R31", "A2=", "R20", "R13", "a3=",
    "R22", "A3x", "M1=", "R23", "R30", "A3=", "R33", "M2x", "M1x", "M2=", "R32", "M3=",
    "M3x",
)
INNER_ORDER = (
    "O3", "a0=", "a2=", "O1", "a1x", "a3x", "O2", "O0", "R01", "a0x", "a3=", "A1x",
    "R21", "A2=", "R00", "A3x", "a2x", "R03", "R31", "R20", "A0x", "R22", "R23", "R02",
    "A0=", "M2=", "M1x", "R30", "A2x", "L31", "R33", "A3=", "R32", "M0x", "M3=", "M0=", "M2x",
    "M3x",
)


LINED = (1,)
BACK_ORDER = ((3, 3), (2, 0), (1, 2), (0, 1))


def mm(former, latter):
    return jnp.dot(former, latter, preferred_element_type=jnp.float32)


def step_kernel(slot_ref, acts_ref, cot_ref, stat_ref, out_ref, new_ref,
                stage, quarters, wholes, acts_all, cot_all, total, stats, direction, left_root, held_ref,
                a_send, a_recv, sib_send, sib_recv, y_send, y_recv, fwd_send, fwd_recv,
                own_send, z_send, x_send, c_recv, quarter_sem, whole_sem, cot_sem, stat_sem,
                back_send, back_recv, owner_ref, owner_sem, line_send):
    dp_count, tokens, blk = acts_all.shape
    mp_count = lax.axis_size("mp")
    part = tokens // mp_count
    chunk = tokens // CHUNKS
    me = lax.axis_index("dp")
    mine = lax.axis_index("mp")
    z, x = me // LANES, me % LANES
    half = z // (DEPTH // 2)
    sign = 1 - 2 * half
    level = half * (DEPTH - 1) + sign * z
    sibling = mine + 1 - 2 * (mine % 2)
    beside = (mine + 2) % mp_count
    across = beside + 1 - 2 * (beside % 2)

    def part_rows(m):
        return pl.ds(pl.multiple_of(m * part, part), part)

    my_rows, beside_rows = part_rows(mine), part_rows(beside)
    sibling_rows, across_rows = part_rows(sibling), part_rows(across)

    def line(i):
        return half * (DEPTH - 1) + sign * i

    def at(i, other):
        return line(i) * LANES + (1 - x if other else x)

    others = [(me + step) % dp_count for step in range(1, dp_count)]
    greeted = [(d, mine) for d in others] + [(me, m) for m in (sibling, beside, across)]
    barrier = pltpu.get_barrier_semaphore()
    for d, m in greeted:
        pl.semaphore_signal(barrier, inc=1, device_id={"dp": d, "mp": m}, device_id_type=MESH)

    cot_load = pltpu.make_async_copy(cot_ref, cot_all.at[me], cot_sem)
    cot_load.start()
    owner_load = pltpu.make_async_copy(slot_ref, owner_ref, owner_sem)
    owner_load.start()
    quarter_loads, whole_loads = [], []
    for w in range(dp_count):
        cols = pl.ds(w * blk, blk)
        quarter_loads.append(pltpu.make_async_copy(acts_ref.at[my_rows, cols], quarters.at[w], quarter_sem.at[w]))
        whole_loads.append(pltpu.make_async_copy(acts_ref.at[:, cols], wholes.at[w], whole_sem.at[w]))
    stat_load = pltpu.make_async_copy(stat_ref, stats, stat_sem)
    for load in quarter_loads + whole_loads + [stat_load]:
        load.start()

    def block_of(d):
        found = 0
        for w in range(dp_count):
            found = jnp.where(owner_ref[w] == d, w, found)
        return found

    def remote(src, dst, send, recv, d, m):
        return pltpu.make_async_remote_copy(
            src_ref=src, dst_ref=dst, send_sem=send, recv_sem=recv,
            device_id={"dp": d, "mp": m}, device_id_type=MESH)

    def arrived(ref, sem):
        pltpu.make_async_copy(ref, ref, sem).wait()

    def cot_piece(who, c):
        return cot_all.at[who, pl.ds(c * chunk, chunk)]

    def own_out(way, c, target):
        return remote(cot_piece(me, c), cot_piece(me, c), own_send.at[way, c], c_recv.at[me, c], target, mine)

    def z_out(i, to, c):
        who = at(i, False)
        return remote(cot_piece(who, c), cot_piece(who, c), z_send.at[i, c], c_recv.at[who, c], at(to, False), mine)

    def x_out(i, c):
        who = at(i, False)
        return remote(cot_piece(who, c), cot_piece(who, c), x_send.at[i, c], c_recv.at[who, c], me + 1 - 2 * x, mine)

    def acts_out(d):
        return remote(stage.at[d], acts_all.at[me, my_rows], a_send.at[d], a_recv.at[me], d, mine)

    def side_out(s, side):
        piece = acts_all.at[s, my_rows]
        return remote(piece, piece, (sib_send, y_send, fwd_send)[side].at[s], (sib_recv, y_recv, fwd_recv)[side].at[s],
                      me, (sibling, beside, across)[side])

    def own_outs(lev, c):
        copies = [own_out(0, c, at(lev + 1, False))]
        if lev > 0:
            copies.append(own_out(1, c, at(lev - 1, False)))
        return copies + [own_out(2, c, me + 1 - 2 * x)]

    def lined_out(c):
        who = at(DEPTH - 1, True)
        return remote(cot_piece(who, c), cot_piece(who, c), line_send.at[c], c_recv.at[who, c], at(0, False), mine)

    def relays(lev, i, c):
        if lev == 0 and i == DEPTH - 1 and c in LINED:
            return []
        copies = [x_out(i, c)]
        if lev > 0:
            copies.append(z_out(i, lev + 1 if i < lev else lev - 1, c))
        return copies

    def by_level(act):
        for lev in range(DEPTH // 2):
            @pl.when(level == lev)
            def _(lev=lev):
                act(lev)

    def start(copies):
        for copy in copies:
            copy.start()

    def handle(word, lev):
        kind, i, which = word[0], int(word[1]), word[2:]
        if kind == "O":
            start(own_outs(lev, i))
        elif kind == "R":
            who = at(i, False)
            arrived(cot_piece(who, int(which)), c_recv.at[who, int(which)])
            start(relays(lev, i, int(which)))
        elif kind == "L":
            who = at(i, True)
            arrived(cot_piece(who, int(which)), c_recv.at[who, int(which)])
            start([lined_out(int(which))])
        else:
            s = at(i, which == "x")
            if kind == "a":
                start([acts_out(s)])
            elif kind == "A":
                arrived(acts_all.at[s, my_rows], a_recv.at[s])
                start([side_out(s, side) for side in (1, 2, 0)])
            else:
                arrived(acts_all.at[s, sibling_rows], sib_recv.at[s])
                arrived(acts_all.at[s, beside_rows], y_recv.at[s])
                arrived(acts_all.at[s, across_rows], fwd_recv.at[s])
                if which == "x":
                    for c in range(CHUNKS):
                        if lev == 0 or i < DEPTH - 1 or c not in LINED:
                            arrived(cot_piece(s, c), c_recv.at[s, c])

    def parts_of(order):
        head = next(n for n, word in enumerate(order) if word[0] != "O")
        wait = next(n for n, word in enumerate(order) if word[0] in "RAM")
        found, now = [order[:head], order[head:wait]], []
        for word in order[wait:]:
            now.append(word)
            if word[0] == "M":
                found.append(now)
                now = []
        return found

    plans = [parts_of(END_ORDER), parts_of(INNER_ORDER)]

    def run_part(n):
        by_level(lambda lev: [handle(word, lev) for word in plans[lev][n]])

    def blend(end, inner):
        return end + (inner - end) * level

    def term_of(n):
        words = [plan[n][-1] for plan in plans]
        place = blend(*[int(word[1]) for word in words])
        other = blend(*[int(word[2] == "x") for word in words])
        return line(place) * LANES + x + (1 - 2 * x) * other

    def product(s):
        return lax.dot_general(acts_all[s], cot_all[s], (((0,), (0,)), ((), ())),
                               preferred_element_type=jnp.float32)

    cot_load.wait()
    pl.semaphore_wait(barrier, len(greeted))
    run_part(0)
    for load in quarter_loads + [owner_load]:
        load.wait()
    for d in range(dp_count):
        stage[d] = quarters[block_of(d)]
    run_part(1)
    for load in whole_loads:
        load.wait()
    acts_all[me] = wholes[block_of(me)]
    total[...] = product(me)
    for n in range(2, dp_count + 1):
        run_part(n)
        total[...] = total[...] + product(term_of(n))

    grad = total[...].astype(jnp.bfloat16)
    stat_load.wait()
    left_root[...], right_root = roots_of(grad, stats, new_ref)
    piece = held_ref.shape[1]
    wide = grad.astype(jnp.float32)
    power, reached = jnp.sum(wide * wide, axis=(0, 1), keepdims=True), 0.0

    def rows_of(d, count=1):
        return pl.ds(pl.multiple_of(d * piece, piece), count * piece)

    planes = [line(blend(*pair)) for pair in BACK_ORDER]
    aims = []
    for plane in planes:
        aims.append(mm(mm(left_root[rows_of(plane * LANES, LANES)], grad).astype(jnp.bfloat16), right_root))
        reached = reached + jnp.sum(aims[-1] * aims[-1], axis=(0, 1), keepdims=True)
    gain = jnp.sqrt((power / wide.size + EPSILON) / (reached / wide.size + EPSILON))
    copies = []
    for n, plane in enumerate(planes):
        direction[rows_of(plane * LANES, LANES)] = (aims[n] * gain).astype(jnp.bfloat16)
        for d in ([plane * LANES + lane for lane in range(LANES)] if n + 1 < DEPTH else [me + 1 - 2 * x]):
            copies.append(remote(direction.at[rows_of(d)], held_ref.at[me], back_send.at[d], back_recv.at[me], d, mine))
            copies[-1].start()
    held_ref[me] = direction[rows_of(me)]

    def sent(lev):
        for c in range(CHUNKS):
            for copy in own_outs(lev, c) + [copy for i in range(DEPTH) if i != lev for copy in relays(lev, i, c)]:
                copy.wait_send()
        for c in LINED if lev else ():
            lined_out(c).wait_send()

    by_level(sent)
    for s in others:
        acts_out(s).wait_send()
        for side in range(3):
            side_out(s, side).wait_send()
    for d in others:
        arrived(held_ref.at[d], back_recv.at[d])
    for w in range(dp_count):
        out_ref[w] = held_ref[owner_ref[w]]
    for copy in copies:
        copy.wait_send()


def roots_of(grad, stat_ref, new_ref):
    low = jnp.bfloat16
    blk = grad.shape[0]
    half = blk // 2
    row = lax.broadcasted_iota(jnp.int32, (half, half), 0)
    col = lax.broadcasted_iota(jnp.int32, (half, half), 1)
    diagonal = row == col

    def whole(parts):
        near, cross, far = [part.astype(low) for part in parts]
        return jnp.concatenate([jnp.concatenate([near, cross], 1), jnp.concatenate([cross.T, far], 1)], 0)

    def product(former, latter):
        right = mm(former, latter[:, half:])
        return mm(former[:half], latter[:, :half]), right[:half], right[half:]

    def gram(rows):
        def part(a, b):
            return lax.dot_general(a, b, (((1,), (1,)), ((), ())), preferred_element_type=jnp.float32)

        top = part(rows[:half], rows)
        return top[:, :half], top[:, half:], part(rows[half:], rows[half:])

    def gram_t(cols):
        def part(a, b):
            return lax.dot_general(a, b, (((0,), (0,)), ((), ())), preferred_element_type=jnp.float32)

        top = part(cols[:, :half], cols)
        return top[:, :half], top[:, half:], part(cols[:, half:], cols[:, half:])

    def total_of(parts):
        near, cross, far = [jnp.sum(part * part, axis=(0, 1), keepdims=True) for part in parts]
        return near + 2.0 * cross + far

    spots = [(slice(0, half), slice(0, half)), (slice(0, half), slice(half, blk)), (slice(half, blk), slice(half, blk))]
    moments, results, scales = [], [None, None], []
    for side, grams in enumerate((gram(grad), gram_t(grad))):
        fresh = [BETA * stat_ref[side, r, c] + (1.0 - BETA) * part for (r, c), part in zip(spots, grams)]
        for (r, c), part in zip(spots, fresh):
            new_ref[side, r, c] = part
        new_ref[side, half:, :half] = fresh[1].T
        shift = jnp.where(diagonal, DAMPING, 0.0)
        damped = [fresh[0] + shift, fresh[1], fresh[2] + shift]
        frob = jnp.sqrt(total_of(damped) + EPSILON)
        scales.append(lax.rsqrt(jnp.sqrt(frob)))
        moments.append([part * (1.0 / frob) for part in damped])
    for iteration in range(ITERS):
        five = jnp.where(diagonal, 5.0, 0.0)
        factors = [[(five - m[0]) * 0.25, m[1] * -0.25, (five - m[2]) * 0.25] for m in moments]
        lows = [whole(factor) for factor in factors]
        if iteration + 1 < ITERS:
            squares = [whole(product(lows[side], lows[side])) for side in range(2)]
            inner = [whole(product(squares[side], whole(moments[side]))) for side in range(2)]
            moments = [product(squares[side], inner[side]) for side in range(2)]
        for side in range(2):
            results[side] = factors[side] if iteration == 0 else product(whole(results[side]), lows[side])
    return [whole([part * scales[side] for part in results[side]]) for side in range(2)]


def owned_step(owner_slot, acts, cotangent, stat_pair, dp_count, mp_count):
    tokens, blk = cotangent.shape
    low, dma = jnp.bfloat16, pltpu.SemaphoreType.DMA
    vmem, hbm = pl.BlockSpec(memory_space=pltpu.VMEM), pl.BlockSpec(memory_space=pltpu.HBM)
    return pl.pallas_call(
        step_kernel,
        name="owned_step",
        out_shape=(jax.ShapeDtypeStruct((dp_count, blk // dp_count, blk), low),
                   jax.ShapeDtypeStruct(stat_pair.shape, jnp.float32)),
        in_specs=[hbm, hbm, hbm, hbm],
        out_specs=(vmem, vmem),
        scratch_shapes=[
            pltpu.VMEM((dp_count, tokens // mp_count, blk), low),
            pltpu.VMEM((dp_count, tokens // mp_count, blk), low),
            pltpu.VMEM((dp_count, tokens, blk), low),
            pltpu.VMEM((dp_count, tokens, blk), low),
            pltpu.VMEM((dp_count, tokens, blk), low),
            pltpu.VMEM((blk, blk), jnp.float32),
            pltpu.VMEM(stat_pair.shape, jnp.float32),
            pltpu.VMEM((blk, blk), low),
            pltpu.VMEM((blk, blk), low),
            pltpu.VMEM((dp_count, blk // dp_count, blk), low),
        ] + [dma((dp_count,))] * 8 + [dma((3, CHUNKS)), dma((DEPTH, CHUNKS)), dma((DEPTH, CHUNKS)),
                                     dma((dp_count, CHUNKS)), dma((dp_count,)), dma((dp_count,)), dma, dma,
                                     dma((dp_count,)), dma((dp_count,)),
                                     pltpu.SMEM(owner_slot.shape, jnp.int32), dma, dma((CHUNKS,))],
        compiler_params=pltpu.CompilerParams(collective_id=0, has_side_effects=True,
                                             vmem_limit_bytes=48 * 1024 * 1024),
    )(*[pltpu.with_memory_space_constraint(a, pltpu.HBM) for a in (owner_slot, acts, cotangent, stat_pair)])


def place_kernel(rows_ref, pair_ref, out_ref, new_ref, rows_sem, pair_sem):
    copies = [pltpu.make_async_copy(pair_ref, new_ref, pair_sem), pltpu.make_async_copy(rows_ref, out_ref, rows_sem)]
    for copy in copies:
        copy.start()
    for copy in copies:
        copy.wait()


def place(rows, new_pair):
    vmem, hbm = pl.BlockSpec(memory_space=pltpu.VMEM), pl.BlockSpec(memory_space=pltpu.HBM)
    return pl.pallas_call(
        place_kernel,
        name="place",
        out_shape=(jax.ShapeDtypeStruct(rows.shape, rows.dtype),
                   jax.ShapeDtypeStruct(new_pair.shape, new_pair.dtype)),
        in_specs=[vmem, vmem],
        out_specs=(hbm, hbm),
        scratch_shapes=[pltpu.SemaphoreType.DMA, pltpu.SemaphoreType.DMA],
        compiler_params=pltpu.CompilerParams(vmem_limit_bytes=4 * 1024 * 1024),
    )(rows, new_pair)


def full_house(acts, cotangent, stats, owner_slot):
    dp_count, mp_count = lax.axis_size("dp"), lax.axis_size("mp")
    rows, new_pair = owned_step(owner_slot, acts, cotangent, stats[0, 0], dp_count, mp_count)
    update, new_pair = place(rows, new_pair)
    return update, new_pair[None, None]


def device_body(acts, cotangent, stats, owner_slot):
    dp_count, mp_count = lax.axis_size("dp"), lax.axis_size("mp")
    blk = cotangent.shape[1]
    every_slot_filled = stats.shape[1] == 1 and acts.shape[1] == dp_count * blk
    if every_slot_filled and mp_count == 4 and dp_count == LANES * DEPTH:
        return full_house(acts, cotangent, stats, owner_slot)
    return on_device(acts, cotangent, stats, owner_slot)


def solution(mesh):
    return jax.shard_map(
        device_body,
        mesh=mesh,
        in_specs=(P("dp", None), P("dp", "mp"), P("mp", "dp", None, None, None), P()),
        out_specs=(P(None, "dp", "mp"), P("mp", "dp", None, None, None)),
        check_vma=False,
    )
```
